16 devices in a mesh: dp: 2 (over z), tp: 8 (over y, x, core).
Axes of the slice: x: 2, y: 2, z: 2, core: 2. Of those that a mesh axis runs over, the one named last changes fastest.
Arguments:
- x: bfloat16 [8192, 4096], P(('dp', 'tp'))
- dy: bfloat16 [8192, 4096], P(('dp', 'tp'))
- u: bfloat16 [8192, 16384], P('dp', 'tp')
- w1: bfloat16 [4096, 16384], P(None, 'tp')
- w2: bfloat16 [16384, 4096], P('tp')
Outputs:
- output 1: bfloat16 [8192, 4096], P(('dp', 'tp'))
- output 2: float32 [4096, 16384], P('dp', 'tp')
- output 3: float32 [16384, 4096], P('tp', 'dp')
All inputs are finite; a program needn't handle non-finite values.
Results may differ from the reference program's by a relative error of at most 0.001.
Values are sent between devices in bfloat16 or wider.
A program may use at most 1 GiB of HBM per device.

```python
import math
import jax
import jax.numpy as jnp

N_ROWS = 8192
HIDDEN = 4096
FFN = 16384


def _gelu(u):
    c = math.sqrt(2.0 / math.pi)
    t = jnp.tanh(c * (u + 0.044715 * u * u * u))
    y = 0.5 * u * (1.0 + t)
    d = 0.5 * (1.0 + t) + 0.5 * u * (1.0 - t * t) * c * (1.0 + 3.0 * 0.044715 * u * u)
    return y, d


def setup_inputs(seed: int = 0) -> dict:
    k = jax.random.split(jax.random.PRNGKey(seed), 5)
    x = jax.random.normal(k[0], (N_ROWS, HIDDEN), jnp.float32).astype(jnp.bfloat16)
    dy = jax.random.normal(k[1], (N_ROWS, HIDDEN), jnp.float32).astype(jnp.bfloat16)
    u = jax.random.normal(k[2], (N_ROWS, FFN), jnp.float32).astype(jnp.bfloat16)
    w1 = (jax.random.normal(k[3], (HIDDEN, FFN), jnp.float32) * HIDDEN ** -0.5).astype(jnp.bfloat16)
    w2 = (jax.random.normal(k[4], (FFN, HIDDEN), jnp.float32) * FFN ** -0.5).astype(jnp.bfloat16)
    return {'x': x, 'dy': dy, 'u': u, 'w1': w1, 'w2': w2}


def reference(x, dy, u, w1, w2):
    y, d = _gelu(u.astype(jnp.float32))
    z = y.astype(jnp.bfloat16)
    dw2 = jnp.dot(z.T, dy, preferred_element_type=jnp.float32)
    g = jnp.dot(dy, w2.T, preferred_element_type=jnp.float32)
    dz = (g * d).astype(jnp.bfloat16)
    dx = jnp.dot(dz, w1.T, preferred_element_type=jnp.float32).astype(jnp.bfloat16)
    dw1 = jnp.dot(x.T, dz, preferred_element_type=jnp.float32)
    return (dx, dw1, dw2)
```

```python
import functools
import math

import jax
import jax.numpy as jnp
from jax import lax
from jax.experimental import pallas as pl
from jax.experimental.pallas import tpu as pltpu
from jax.sharding import PartitionSpec as P

F32 = jnp.float32
BF16 = jnp.bfloat16
MESH = pl.DeviceIdType.MESH
MIB = 2 ** 20


def _gelu(u):
    c = math.sqrt(2.0 / math.pi)
    t = jnp.tanh(c * (u + 0.044715 * u * u * u))
    y = 0.5 * u * (1.0 + t)
    d = 0.5 * (1.0 + t) + 0.5 * u * (1.0 - t * t) * c * (1.0 + 3.0 * 0.044715 * u * u)
    return y, d


def _dot(a, b, ca, cb):
    return lax.dot_general(a, b, (((ca,), (cb,)), ((), ())), preferred_element_type=F32)


def kernel(x, dy, u, w1, w2, dx, dw1, dw2, dya, dyb, xa, xb, ub, w1s, dza, dzb, dzs, za, zb, da, db, p1, rr, p2, ss,
           send, recv):
    r = lax.axis_index('dp')
    t = lax.axis_index('tp')
    core, xbit, ybit = t % 2, (t // 2) % 2, t // 4
    n, hid = x.shape
    ffn = u.shape[1]
    half = hid // 2
    two = 2 * n

    def chip(fx, fy):
        return (xbit + fx) % 2 + 2 * ((ybit + fy) % 2)

    def shard(fx, fy, fc=0):
        return chip(fx, fy) * 2 + (core + fc) % 2

    peer = {
        'c': {'tp': shard(0, 0, 1)},
        'x': {'tp': shard(1, 0)},
        'y': {'tp': shard(0, 1)},
        'z': {'dp': 1 - r},
    }

    def rows(fx, fy, fc=0, part=None):
        start = shard(fx, fy, fc) * n
        if part is None:
            return pl.ds(pl.multiple_of(start, n), n)
        return pl.ds(pl.multiple_of(start + part * (n // 2), n // 2), n // 2)

    def chip_rows(fx, fy):
        return pl.ds(pl.multiple_of(chip(fx, fy) * two, two), two)

    copies = []

    def push(to, src, dst):
        i = len(copies)
        cp = pltpu.make_async_remote_copy(
            src_ref=src, dst_ref=dst, send_sem=send.at[i], recv_sem=recv.at[i],
            device_id=peer[to], device_id_type=MESH)
        cp.start()
        copies.append(cp)
        return cp

    barrier = pltpu.get_barrier_semaphore()
    for to in peer:
        pl.semaphore_signal(barrier, inc=1, device_id=peer[to], device_id_type=MESH)
    pl.semaphore_wait(barrier, len(peer))

    own = rows(0, 0)
    mine = pl.ds(pl.multiple_of(r * half, half), half)
    other = pl.ds(pl.multiple_of((1 - r) * half, half), half)

    def cast(to, buf, src, where):
        return push(to, src, buf.at[where, :])

    c_dya = {}
    c_dya['own'] = cast('c', dya, dy, own)
    x_dya = cast('x', dya, dy, own)
    y_dya = cast('y', dya, dy, own)
    z_dy = cast('z', dyb, dy, own)
    z_x = cast('z', xb, x.at[:, other], own)
    c_w1 = push('c', w1, w1s)
    c_xa = [cast('c', xa, x.at[:, mine], own)]
    x_xa = cast('x', xa, x.at[:, mine], own)
    y_xa = cast('y', xa, x.at[:, mine], own)
    flips = {'own': (0, 0), 'x': (1, 0), 'y': (0, 1), 'd': (1, 1)}
    z_u = {q: push('z', u.at[chip_rows(*flips[q]), :], ub.at[chip_rows(*flips[q]), :]) for q in flips}

    def copy_body(a, b):
        b[...] = a[...]

    tr = 128
    pltpu.emit_pipeline(
        copy_body, grid=(n // tr,),
        in_specs=[pl.BlockSpec((tr, hid), lambda i: (i, 0))],
        out_specs=[pl.BlockSpec((tr, hid), lambda i: (shard(0, 0) * (n // tr) + i, 0))],
    )(dy, dya)
    pltpu.emit_pipeline(
        copy_body, grid=(n // tr,),
        in_specs=[pl.BlockSpec((tr, half), lambda i: (i, r))],
        out_specs=[pl.BlockSpec((tr, half), lambda i: (shard(0, 0) * (n // tr) + i, 0))],
    )(x, xa)

    def act_body(uu, z, d):
        @pl.loop(0, uu.shape[0] // 16)
        def _(i):
            s = pl.ds(pl.multiple_of(i * 16, 16), 16)
            y, g = _gelu(uu[s, :].astype(F32))
            z[s, :] = y.astype(BF16)
            d[s, :] = g

    def act(src, z, d, flip, count):
        tm = 256
        per = two // tm
        spec = pl.BlockSpec((tm, ffn), lambda i, j: (chip(*flip(i)) * per + j, 0))
        pltpu.emit_pipeline(act_body, grid=(count, per), in_specs=[spec], out_specs=[spec, spec])(src, z, d)

    def g_body(a, w, d, o):
        o[...] = (_dot(a[...], w[...], 1, 1) * d[...]).astype(BF16)

    def g_stage(a, d, o, flip, count):
        tn = 512
        io = pl.BlockSpec((two, tn), lambda i, j: (chip(*flip(i)), j))
        pltpu.emit_pipeline(
            g_body, grid=(count, ffn // tn),
            in_specs=[pl.BlockSpec((two, hid), lambda i, j: (chip(*flip(i)), 0)),
                      pl.BlockSpec((tn, hid), lambda i, j: (j, 0)), io],
            out_specs=[io])(a, w2, d, o)

    def first(i):
        return 0, 0

    def nears(i):
        return 1 - i, i

    def last(i):
        return 1, 1

    act(u, za, da, lambda i: (i % 2, i // 2), 4)
    c_dz = {}

    def swap_dz(q):
        where = rows(*flips[q], 1)
        c_dz[q] = push('c', dza.at[where, :], dzs.at[where, :])

    c_dya['own'].wait_recv()
    g_stage(dya, da, dza, first, 1)
    swap_dz('own')

    x_dya.wait_recv()
    y_dya.wait_recv()
    top, low = 0, 1

    def relay(buf):
        a = push('x', buf.at[rows(0, 1, 0, top), :], buf.at[rows(0, 1, 0, top), :])
        b = push('y', buf.at[rows(1, 0, 0, low), :], buf.at[rows(1, 0, 0, low), :])
        return a, b

    def sib(buf, q):
        where = rows(*flips[q])
        return push('c', buf.at[where, :], buf.at[where, :])

    c_dya['x'] = sib(dya, 'x')
    c_dya['y'] = sib(dya, 'y')
    dya_d = relay(dya)
    z_dy.wait_recv()
    x_dyb = push('x', dyb.at[own, :], dyb.at[own, :])
    y_dyb = push('y', dyb.at[own, :], dyb.at[own, :])
    c_dyb = {'own': sib(dyb, 'own')}
    c_dya['x'].wait_recv()
    c_dya['y'].wait_recv()
    g_stage(dya, da, dza, nears, 2)
    swap_dz('x')
    swap_dz('y')

    x_xa.wait_recv()
    y_xa.wait_recv()
    c_xa += [sib(xa, 'x'), sib(xa, 'y')]
    xa_d = relay(xa)
    for cp in dya_d:
        cp.wait_recv()
    c_dya['d'] = sib(dya, 'd')
    where = rows(1, 1)
    z_dyd = push('z', dya.at[where, :], dyb.at[where, :])
    c_dya['d'].wait_recv()
    g_stage(dya, da, dza, last, 1)
    swap_dz('d')
    c_w1.wait_recv()
    for q in c_dz:
        c_dz[q].wait_recv()

    def p_body(a, b, w, ws, o):
        o[0] = _dot(a[...], w[...], 1, 1) + _dot(b[...], ws[...], 1, 1)

    def p_add_body(a, b, w, ws, s, o):
        o[0] = (_dot(a[...], w[...], 1, 1) + _dot(b[...], ws[...], 1, 1)) + s[0]

    def p_stage(flip, out, add=None):
        tn = 1024
        dz = pl.BlockSpec((n, ffn), lambda h, j, i: (shard(*flip(h, i)), 0))
        w = pl.BlockSpec((tn, ffn), lambda h, j, i: (h * (half // tn) + j, 0))
        o = pl.BlockSpec((1, n, tn), lambda h, j, i: (h * 2 + i, 0, j))
        grid = (2, half // tn, 2)
        if add is None:
            pltpu.emit_pipeline(p_body, grid=grid, in_specs=[dz, dz, w, w], out_specs=[o])(dza, dzs, w1, w1s, out)
        else:
            pltpu.emit_pipeline(p_add_body, grid=grid, in_specs=[dz, dz, w, w, o], out_specs=[o])(
                dza, dzs, w1, w1s, add, out)

    p_stage(lambda h, i: (1 - h * i, h + i - h * i), p1)
    rs1 = [push('xxyy'[i], p1.at[i], rr.at[i]) for i in (0, 1, 2, 3)]
    z_x.wait_recv()
    x_xb = push('x', xb.at[own, :], xb.at[own, :])
    y_xb = push('y', xb.at[own, :], xb.at[own, :])
    c_xb = [sib(xb, 'own')]

    def dw_body(a, b, o):
        k = pl.program_id(2)

        @pl.when(k == 0)
        def _():
            o[...] = _dot(a[...], b[...], 0, 0)

        @pl.when(k > 0)
        def _():
            o[...] += _dot(a[...], b[...], 0, 0)

    def dw_add_body(a, b, s, o):
        k = pl.program_id(2)

        @pl.when(k == 0)
        def _():
            o[...] = s[...] + _dot(a[...], b[...], 0, 0)

        @pl.when(k > 0)
        def _():
            o[...] += _dot(a[...], b[...], 0, 0)

    def dw_stage(a, b, col, out, k0, nk, add):
        tb = 1024
        grid = (2048 // tb, 2048 // tb, nk)
        sa = pl.BlockSpec((two, tb), lambda i, j, k: (chip((k + k0) % 2, (k + k0) // 2), i))
        sb = pl.BlockSpec((two, tb), lambda i, j, k: (chip((k + k0) % 2, (k + k0) // 2), col + j))
        so = pl.BlockSpec((tb, tb), lambda i, j, k: (i, j))
        if add:
            pltpu.emit_pipeline(dw_add_body, grid=grid, in_specs=[sa, sb, so], out_specs=[so])(a, b, out, out)
        else:
            pltpu.emit_pipeline(dw_body, grid=grid, in_specs=[sa, sb], out_specs=[so])(a, b, out)

    ycol = r * (half // 1024)
    dw_stage(za, dya, ycol, dw2, 0, 4, False)

    z_u['own'].wait_recv()
    act(ub, zb, db, first, 1)
    c_dyb['own'].wait_recv()
    g_stage(dyb, db, dzb, first, 1)

    for cp in xa_d:
        cp.wait_recv()
    c_xa.append(sib(xa, 'd'))
    x_dyb.wait_recv()
    y_dyb.wait_recv()
    c_dyb['x'] = sib(dyb, 'x')
    c_dyb['y'] = sib(dyb, 'y')
    for cp in c_xa:
        cp.wait_recv()
    dw_stage(xa, dza, 0, dw1, 0, 4, False)

    z_u['x'].wait_recv()
    z_u['y'].wait_recv()
    act(ub, zb, db, nears, 2)
    c_dyb['x'].wait_recv()
    c_dyb['y'].wait_recv()
    g_stage(dyb, db, dzb, nears, 2)
    for cp in rs1:
        cp.wait_recv()
    p_stage(lambda h, i: (h * (1 - i), (1 - h) * i), p2, rr)
    x_xb.wait_recv()
    y_xb.wait_recv()
    xb_d = relay(xb)
    rs2 = [push('y', p2.at[1], ss.at[0]), push('x', p2.at[2], ss.at[1])]
    c_xb += [sib(xb, 'x'), sib(xb, 'y')]
    dw_stage(zb, dyb, ycol, dw2, 0, 3, True)
    for cp in c_xb:
        cp.wait_recv()
    dw_stage(xb, dzb, 0, dw1, 0, 3, True)

    for cp in xb_d:
        cp.wait_recv()
    c_xbd = sib(xb, 'd')
    z_u['d'].wait_recv()
    act(ub, zb, db, last, 1)
    z_dyd.wait_recv()
    c_dyb['d'] = sib(dyb, 'd')
    c_dyb['d'].wait_recv()
    g_stage(dyb, db, dzb, last, 1)
    dw_stage(zb, dyb, ycol, dw2, 3, 1, True)
    c_xbd.wait_recv()
    dw_stage(xb, dzb, 0, dw1, 3, 1, True)
    for cp in rs2:
        cp.wait_recv()

    def fin_body(a, b, o):
        o[...] = (a[0] + b[0]).astype(BF16)

    tn = 512
    pltpu.emit_pipeline(
        fin_body, grid=(2, half // tn),
        in_specs=[pl.BlockSpec((1, n, tn), lambda h, j: (3 * h, 0, j)),
                  pl.BlockSpec((1, n, tn), lambda h, j: (h, 0, j))],
        out_specs=[pl.BlockSpec((n, tn), lambda h, j: (0, h * (half // tn) + j))],
    )(p2, ss, dx)
    for cp in copies:
        cp.wait_send()


COPIES = 52


def solution(mesh):
    def body(x, dy, u, w1, w2):
        n, hid = x.shape
        rows, ffn = u.shape
        half = hid // 2

        def s(*shape, dtype=BF16):
            return jax.ShapeDtypeStruct(shape, dtype)

        outs = [
            s(n, hid), s(half, ffn, dtype=F32), s(ffn, half, dtype=F32),
            s(rows, hid), s(rows, hid), s(rows, half), s(rows, half), s(rows, ffn), s(hid, ffn),
            s(rows, ffn), s(rows, ffn), s(rows, ffn), s(rows, ffn), s(rows, ffn),
            s(rows, ffn, dtype=F32), s(rows, ffn, dtype=F32),
            s(4, n, half, dtype=F32), s(4, n, half, dtype=F32), s(4, n, half, dtype=F32), s(2, n, half, dtype=F32),
        ]
        got = pl.pallas_call(
            kernel,
            out_shape=outs,
            in_specs=[pl.BlockSpec(memory_space=pl.ANY)] * 5,
            out_specs=[pl.BlockSpec(memory_space=pl.ANY)] * len(outs),
            scratch_shapes=[pltpu.SemaphoreType.DMA((COPIES,)), pltpu.SemaphoreType.DMA((COPIES,))],
            compiler_params=pltpu.CompilerParams(
                collective_id=0, has_side_effects=True, vmem_limit_bytes=60 * MIB),
        )(x, dy, u, w1, w2)
        return tuple(got[:3])

    return jax.shard_map(
        body, mesh=mesh,
        in_specs=(P(('dp', 'tp'), None), P(('dp', 'tp'), None), P('dp', 'tp'), P(None, 'tp'), P('tp', None)),
        out_specs=(P(('dp', 'tp'), None), P('dp', 'tp'), P('tp', 'dp')),
        check_vma=False)
```

```python
import functools
import math

import jax
import jax.numpy as jnp
from jax import lax
from jax.experimental import pallas as pl
from jax.experimental.pallas import tpu as pltpu
from jax.sharding import PartitionSpec as P

F32 = jnp.float32
BF16 = jnp.bfloat16
MESH = pl.DeviceIdType.MESH
MIB = 2 ** 20


def _gelu(u):
    c = math.sqrt(2.0 / math.pi)
    u2 = u * u
    t = jnp.tanh(u * (c + (c * 0.044715) * u2))
    h = 0.5 * (1.0 + t)
    d = h + (u * h) * ((1.0 - t) * (c + (c * 3.0 * 0.044715) * u2))
    return u * h, d


def _dot(a, b, ca, cb):
    return lax.dot_general(a, b, (((ca,), (cb,)), ((), ())), preferred_element_type=F32)


def kernel(x, dy, u, w1, w2, po, rr, p2, ss, dw1, dw2, xd, dyk, zd, dzd, dyd, dyf, xf, ub, w1s, dzf, dzs, zf, df, gd, p1,
           send, recv):
    r = lax.axis_index('dp')
    t = lax.axis_index('tp')
    core, xbit, ybit = t % 2, (t // 2) % 2, t // 4
    n, hid = x.shape
    local, ffn = u.shape
    half = hid // 2
    two = 2 * n
    bit = n // 16

    def chip(fx, fy):
        return (xbit + fx) % 2 + 2 * ((ybit + fy) % 2)

    def shard(fx, fy, fc=0):
        return chip(fx, fy) * 2 + (core + fc) % 2

    peer = {
        'c': {'tp': shard(0, 0, 1)},
        'x': {'tp': shard(1, 0)},
        'y': {'tp': shard(0, 1)},
        'z': {'dp': 1 - r},
    }
    flips = {'own': (0, 0), 'x': (1, 0), 'y': (0, 1), 'd': (1, 1)}

    def rows(q, plane=0, fc=0, lo=0, size=None):
        start = plane * local + shard(*flips[q], fc) * n + lo
        return pl.ds(pl.multiple_of(start, bit), n if size is None else size)

    def chip_rows(q, lo=0, size=two):
        return pl.ds(pl.multiple_of(chip(*flips[q]) * two + lo, n), size)

    def mine_of(lo=0, size=None):
        return pl.ds(pl.multiple_of(core * n + lo, bit), n if size is None else size)

    copies = []

    def push(to, src, dst):
        i = len(copies)
        cp = pltpu.make_async_remote_copy(
            src_ref=src, dst_ref=dst, send_sem=send.at[i], recv_sem=recv.at[i],
            device_id=peer[to], device_id_type=MESH)
        cp.start()
        copies.append(cp)
        return cp

    barrier = pltpu.get_barrier_semaphore()
    for to in peer:
        pl.semaphore_signal(barrier, inc=1, device_id=peer[to], device_id_type=MESH)
    pl.semaphore_wait(barrier, len(peer))

    own, own1 = rows('own'), rows('own', 1)
    keep = pl.ds(pl.multiple_of(r * half, half), half)
    give = pl.ds(pl.multiple_of((1 - r) * half, half), half)

    x_dy = push('x', dy, dyf.at[own, :])
    y_dy = push('y', dy, dyf.at[own, :])
    z_dy = push('z', dy, dyf.at[own1, :])
    c_dy = push('c', dy, dyf.at[own, :])
    z_x = push('z', x.at[:, give], xf.at[own1, :])
    x_x = push('x', x.at[:, keep], xf.at[own, :])
    y_x = push('y', x.at[:, keep], xf.at[own, :])
    c_w1 = push('c', w1, w1s)
    c_x = [push('c', x.at[:, keep], xf.at[own, :])]

    def push_u(q, lo=0, size=two):
        where = chip_rows(q, lo, size)
        return push('z', u.at[where, :], ub.at[where, :])

    z_u = {'own': push_u('own'), 'x': push_u('x')}

    def copy_body(a, b):
        b[...] = a[...]

    tr = 128
    pltpu.emit_pipeline(
        copy_body, grid=(n // tr,),
        in_specs=[pl.BlockSpec((tr, hid), lambda i: (i, 0))],
        out_specs=[pl.BlockSpec((tr, hid), lambda i: (shard(0, 0) * (n // tr) + i, 0))],
    )(dy, dyf)
    pltpu.emit_pipeline(
        copy_body, grid=(n // tr,),
        in_specs=[pl.BlockSpec((tr, half), lambda i: (i, r))],
        out_specs=[pl.BlockSpec((tr, half), lambda i: (shard(0, 0) * (n // tr) + i, 0))],
    )(x, xf)

    def act_body(uu, z, d):
        @pl.loop(0, uu.shape[0] // 16)
        def _(i):
            s = pl.ds(pl.multiple_of(i * 16, 16), 16)
            y, g = _gelu(uu[s, :].astype(F32))
            z[s, :] = y.astype(BF16)
            d[s, :] = g

    def act_mul_body(uu, g, z, dz):
        @pl.loop(0, uu.shape[0] // 16)
        def _(i):
            s = pl.ds(pl.multiple_of(i * 16, 16), 16)
            y, d = _gelu(uu[s, :].astype(F32))
            z[s, :] = y.astype(BF16)
            dz[s, :] = (g[s, :] * d).astype(BF16)

    tm = 256
    per = two // tm

    def act(src, plane, flip, count):
        ins = pl.BlockSpec((tm, ffn), lambda i, j: (chip(*flip(i)) * per + j, 0))
        out = pl.BlockSpec((tm, ffn), lambda i, j: ((4 * plane + chip(*flip(i))) * per + j, 0))
        pltpu.emit_pipeline(act_body, grid=(count, per), in_specs=[ins], out_specs=[out, out])(src, zf, df)

    def act_last(part):
        base = part * (n // tm)
        ins = pl.BlockSpec((tm, ffn), lambda j: (chip(1, 1) * per + base + j, 0))
        io = pl.BlockSpec((tm, ffn), lambda j: (base + j, 0))
        pltpu.emit_pipeline(
            act_mul_body, grid=(n // tm,), in_specs=[ins, io], out_specs=[io, io])(ub, gd, zd, dzd)

    def g_body(a, w, d, o):
        @pl.loop(0, 2)
        def _(i):
            s = pl.ds(pl.multiple_of(i * n, n), n)
            o[s, :] = (_dot(a[s, :], w[...], 1, 1) * d[s, :]).astype(BF16)

    def g32_body(a, w, o):
        @pl.loop(0, 2)
        def _(i):
            s = pl.ds(pl.multiple_of(i * n, n), n)
            o[s, :] = _dot(a[s, :], w[...], 1, 1)

    def g_stage(plane, flip, count):
        tn = 512
        io = pl.BlockSpec((two, tn), lambda i, j: (4 * plane + chip(*flip(i)), j))
        pltpu.emit_pipeline(
            g_body, grid=(count, ffn // tn),
            in_specs=[pl.BlockSpec((two, hid), lambda i, j: (4 * plane + chip(*flip(i)), 0)),
                      pl.BlockSpec((tn, hid), lambda i, j: (j, 0)), io],
            out_specs=[io])(dyf, w2, df, dzf)

    def g32_stage():
        tn = 512
        pltpu.emit_pipeline(
            g32_body, grid=(ffn // tn,),
            in_specs=[pl.BlockSpec((two, hid), lambda j: (0, 0)), pl.BlockSpec((tn, hid), lambda j: (j, 0))],
            out_specs=[pl.BlockSpec((two, tn), lambda j: (0, j))])(dyd, w2, gd)

    def strips(fn):
        @pl.loop(0, 2)
        def _(i):
            fn(pl.ds(pl.multiple_of(i * 512, 512), 512))

    def dw_body(a, b, o):
        k = pl.program_id(2)

        def set_to(s):
            o[s, :] = _dot(a[:, s], b[...], 0, 0)

        def add_to(s):
            o[s, :] += _dot(a[:, s], b[...], 0, 0)

        pl.when(k == 0)(lambda: strips(set_to))
        pl.when(k > 0)(lambda: strips(add_to))

    def dw_add_body(a, b, c, o):
        k = pl.program_id(2)

        def set_to(s):
            o[s, :] = c[s, :] + _dot(a[:, s], b[...], 0, 0)

        def add_to(s):
            o[s, :] += _dot(a[:, s], b[...], 0, 0)

        pl.when(k == 0)(lambda: strips(set_to))
        pl.when(k > 0)(lambda: strips(add_to))

    def dw_one_body(a, b, c, o):
        def set_to(s):
            o[s, :] = c[s, :] + _dot(a[:, s], b[...], 0, 0)

        strips(set_to)

    def dw_stage(a, b, col, out, k0, nk, add):
        tb = 1024
        grid = (2048 // tb, 2048 // tb, nk)

        def at(k):
            m = k + k0
            return 4 * (m // 4) + chip(m % 2, (m % 4) // 2)

        sa = pl.BlockSpec((two, tb), lambda i, j, k: (at(k), i))
        sb = pl.BlockSpec((two, tb), lambda i, j, k: (at(k), col + j))
        so = pl.BlockSpec((tb, tb), lambda i, j, k: (i, j))
        if add:
            pltpu.emit_pipeline(dw_add_body if nk > 1 else dw_one_body, grid=grid, in_specs=[sa, sb, so], out_specs=[so])(a, b, out, out)
        else:
            pltpu.emit_pipeline(dw_body, grid=grid, in_specs=[sa, sb], out_specs=[so])(a, b, out)

    def p_body(a, b, w, ws, o):
        o[0] = _dot(a[...], w[...], 1, 1) + _dot(b[...], ws[...], 1, 1)

    def p_add_body(a, b, w, ws, s, o):
        o[0] = (_dot(a[...], w[...], 1, 1) + _dot(b[...], ws[...], 1, 1)) + s[0]

    def p_stage(flip, count, out, add=None):
        tn = 1024
        dz = pl.BlockSpec((n, ffn), lambda h, j, i: (shard(*flip(h, i)), 0))
        w = pl.BlockSpec((tn, ffn), lambda h, j, i: (h * (half // tn) + j, 0))
        o = pl.BlockSpec((1, n, tn), lambda h, j, i: (h * count + i, 0, j))
        grid = (2, half // tn, count)
        if add is None:
            pltpu.emit_pipeline(p_body, grid=grid, in_specs=[dz, dz, w, w], out_specs=[o])(dzf, dzs, w1, w1s, out)
        else:
            got = pl.BlockSpec((1, n, tn), lambda h, j, i: (1 + h, 0, j))
            pltpu.emit_pipeline(p_add_body, grid=grid, in_specs=[dz, dz, w, w, got], out_specs=[o])(
                dzf, dzs, w1, w1s, add, out)

    def only(q):
        return lambda i: flips[q]

    def nears(i):
        return 1 - i, i

    def sib(buf, q, plane=0):
        where = rows(q, plane)
        return push('c', buf.at[where, :], buf.at[where, :])

    c_dz = []

    def swap_dz(q):
        where = rows(q, 0, 1)
        c_dz.append(push('c', dzf.at[where, :], dzs.at[where, :]))

    def relay(buf, plane, dst=None):
        out = []
        for to, q, lo in (('x', 'y', 0), ('y', 'x', n // 2)):
            where = rows(q, plane, 0, lo, n // 2)
            there = buf.at[where, :] if dst is None else dst.at[mine_of(lo, n // 2), :]
            out.append(push(to, buf.at[where, :], there))
        return out

    act(u, 0, lambda i: (i % 2, i // 2), 4)
    c_dy.wait_recv()
    g_stage(0, only('own'), 1)
    swap_dz('own')
    c_w1.wait_recv()
    c_dz.pop().wait_recv()
    p_stage(lambda h, i: (0, 0), 1, po)

    x_dy.wait_recv()
    y_dy.wait_recv()
    c_near = [sib(dyf, 'x'), sib(dyf, 'y')]
    dy_d = relay(dyf, 0)
    z_bits = []
    for q in ('x', 'y'):
        z_bits.append(push('z', dyf.at[rows(q, 0, 0, 0, bit), :], dyf.at[rows(q, 1, 0, 0, bit), :]))
    z_dy.wait_recv()
    rest = rows('own', 1, 0, bit, n - bit)
    dyb = [push(to, dyf.at[rest, :], dyf.at[rest, :]) for to in 'xy']
    c_dyb = sib(dyf, 'own', 1)
    for cp in c_near:
        cp.wait_recv()
    g_stage(0, nears, 2)
    swap_dz('x')
    swap_dz('y')

    x_x.wait_recv()
    y_x.wait_recv()
    c_x += [sib(xf, 'x'), sib(xf, 'y')]
    x_d = relay(xf, 0)
    ycol = r * (half // 1024)
    dw_stage(zf, dyf, ycol, dw2, 0, 3, False)

    for cp in dy_d:
        cp.wait_recv()
    c_dyd = sib(dyf, 'd')
    z_dyd = push('z', dyf.at[rows('d'), :], dyd.at[mine_of(), :])
    z_u['y'] = push_u('y')
    z_ud = [push_u('d', 0, n), push_u('d', n, n)]
    c_dyd.wait_recv()
    g_stage(0, only('d'), 1)
    swap_dz('d')
    for cp in c_dz:
        cp.wait_recv()
    p_stage(lambda h, i: (1 - h * i, h + i - h * i), 2, p1)
    rs1 = [push('xxyy'[i], p1.at[i], rr.at[i]) for i in (0, 1, 2, 3)]
    z_x.wait_recv()
    xb = [push(to, xf.at[own1, :], xf.at[own1, :]) for to in 'xy']
    c_xb = [sib(xf, 'own', 1)]

    z_u['own'].wait_recv()
    act(ub, 1, only('own'), 1)
    c_dyb.wait_recv()
    g_stage(1, only('own'), 1)
    for cp in x_d:
        cp.wait_recv()
    c_x.append(sib(xf, 'd'))
    for cp in dyb + z_bits:
        cp.wait_recv()
    c_dyb = [sib(dyf, 'x', 1), sib(dyf, 'y', 1)]
    for cp in c_x + c_xb:
        cp.wait_recv()
    dw_stage(xf, dzf, 0, dw1, 0, 5, False)

    z_u['x'].wait_recv()
    act(ub, 1, only('x'), 1)
    for cp in c_dyb:
        cp.wait_recv()
    g_stage(1, only('x'), 1)
    dw_stage(zf, dyf, ycol, dw2, 3, 3, True)
    z_dyd.wait_recv()
    c_dyd = push('c', dyd.at[mine_of(), :], dyd.at[mine_of(), :])
    c_dyd.wait_recv()
    g32_stage()
    pltpu.emit_pipeline(
        copy_body, grid=(two // tr,),
        in_specs=[pl.BlockSpec((tr, half), lambda i: (i, r))],
        out_specs=[pl.BlockSpec((tr, half), lambda i: (i, 0))])(dyd, dyk)
    for cp in rs1:
        cp.wait_recv()
    p_stage(lambda h, i: (h, 1 - h), 1, p2, rr)
    for cp in xb:
        cp.wait_recv()
    xb_d = relay(xf, 1, xd)
    early = pl.ds(0, ss.shape[2])
    rs2 = [push('y', p2.at[0, :, early], ss.at[0]), push('x', p2.at[1, :, early], ss.at[1])]
    c_xb = [sib(xf, 'x', 1), sib(xf, 'y', 1)]
    z_u['y'].wait_recv()
    act(ub, 1, only('y'), 1)
    g_stage(1, only('y'), 1)
    dw_stage(zf, dyf, ycol, dw2, 6, 1, True)
    for cp in c_xb:
        cp.wait_recv()
    dw_stage(xf, dzf, 0, dw1, 5, 2, True)

    for cp in xb_d:
        cp.wait_recv()
    c_xd = push('c', xd.at[mine_of(), :], xd.at[mine_of(), :])
    z_ud[0].wait_recv()
    act_last(0)
    z_ud[1].wait_recv()
    act_last(1)
    c_xd.wait_recv()
    for cp in rs2:
        cp.wait_recv()
    for cp in copies:
        cp.wait_send()


def finish(po, rr, ss, ty, tx, dx):
    tm = 128
    n, half = po.shape[1:]
    cut = ss.shape[2]

    def body(a, b, c, ey, ex, o):
        o[:, :cut] = ((a[0, :, :cut] + b[0, :, :cut]) + c[0]).astype(BF16)
        side = a[0, :, cut:] + b[0, :, cut:]

        @pl.when(pl.program_id(0) == 0)
        def _():
            o[:, cut:] = (side + ey[...]).astype(BF16)

        @pl.when(pl.program_id(0) == 1)
        def _():
            o[:, cut:] = (side + ex[...]).astype(BF16)

    end = pl.BlockSpec((tm, half - cut), lambda h, i: (i, 0))
    pltpu.emit_pipeline(
        body, grid=(2, n // tm),
        in_specs=[pl.BlockSpec((1, tm, half), lambda h, i: (h, i, 0)),
                  pl.BlockSpec((1, tm, half), lambda h, i: (3 * h, i, 0)),
                  pl.BlockSpec((1, tm, cut), lambda h, i: (h, i, 0)), end, end],
        out_specs=[pl.BlockSpec((tm, half), lambda h, i: (i, h))])(po, rr, ss, ty, tx, dx)


COPIES = 56


def solution(mesh):
    def body(x, dy, u, w1, w2):
        n, hid = x.shape
        rows, ffn = u.shape
        half = hid // 2
        late = half * 3 // 8

        def s(*shape, dtype=BF16):
            return jax.ShapeDtypeStruct(shape, dtype)

        outs = [
            s(2, n, half, dtype=F32), s(4, n, half, dtype=F32), s(2, n, half, dtype=F32),
            s(2, n, half - late, dtype=F32), s(half, ffn, dtype=F32), s(ffn, half, dtype=F32),
            s(2 * n, half), s(2 * n, half), s(2 * n, ffn), s(2 * n, ffn), s(2 * n, hid),
            s(2 * rows, hid), s(2 * rows, half), s(rows, ffn), s(hid, ffn),
            s(2 * rows, ffn), s(rows, ffn), s(2 * rows, ffn), s(2 * rows, ffn, dtype=F32), s(2 * n, ffn, dtype=F32),
            s(4, n, half, dtype=F32),
        ]
        got = pl.pallas_call(
            kernel,
            out_shape=outs,
            in_specs=[pl.BlockSpec(memory_space=pl.ANY)] * 5,
            out_specs=[pl.BlockSpec(memory_space=pl.ANY)] * len(outs),
            scratch_shapes=[pltpu.SemaphoreType.DMA((COPIES,)), pltpu.SemaphoreType.DMA((COPIES,))],
            compiler_params=pltpu.CompilerParams(
                collective_id=0, has_side_effects=True, vmem_limit_bytes=60 * MIB),
        )(x, dy, u, w1, w2)
        po, rr, p2, ss, dw1, dw2, xd, dyk, zd, dzd = got[:10]
        def swap(v, mask):
            return lax.ppermute(v, 'tp', [(i, i ^ mask) for i in range(8)])

        with jax.named_scope('tail_y'):
            ty = swap(p2[0, :, -late:], 4)
        with jax.named_scope('tail_x'):
            tx = swap(p2[1, :, -late:], 2)
        with jax.named_scope('last2'):
            dw2 = dw2 + _dot(zd, dyk, 0, 0)
        with jax.named_scope('last1'):
            dw1 = dw1 + _dot(xd, dzd, 0, 0)
        dx = pl.pallas_call(
            finish, out_shape=s(n, hid),
            in_specs=[pl.BlockSpec(memory_space=pl.ANY)] * 5,
            out_specs=pl.BlockSpec(memory_space=pl.ANY),
            cost_estimate=pl.CostEstimate(flops=n * hid, bytes_accessed=10 * n * hid, transcendentals=0),
            compiler_params=pltpu.CompilerParams(vmem_limit_bytes=60 * MIB),
        )(po, rr, ss, ty, tx)
        return dx, dw1, dw2

    return jax.shard_map(
        body, mesh=mesh,
        in_specs=(P(('dp', 'tp'), None), P(('dp', 'tp'), None), P('dp', 'tp'), P(None, 'tp'), P('tp', None)),
        out_specs=(P(('dp', 'tp'), None), P('dp', 'tp'), P('tp', 'dp')),
        check_vma=False)
```
